32 devices in a mesh: head: 2 (over core), seq: 16 (over z, y, x).
Axes of the slice: x: 2, y: 2, z: 4, core: 2. Of those that a mesh axis runs over, the one named last changes fastest.
Arguments:
- queries: bfloat16 [8192, 4096], P('seq', 'head'), may hold values from -512 to 512
- keys: bfloat16 [8192, 2048], P('seq', 'head'), may hold values from -8 to 8
- values: bfloat16 [8192, 2048], P('seq', 'head'), may hold values from -6 to 6
- episode: int32 [8192], replicated, may hold values from 0 to 7, never falling along the last dimension, each value on 1 to 2048 neighbouring positions
- out_weight: bfloat16 [4096, 4608], P('head'), may hold values from -0.375 to 0.375
Outputs:
- projected: bfloat16 [8192, 4608], P('seq', 'head')
The draws below stay inside these ranges and needn't reach their ends.
Inputs may be any that keep to these rules, and one draw needn't show every extreme that they name: episode numbers never fall along the trajectory.
All inputs are finite; a program needn't handle non-finite values.
Results may differ from the reference program's by a relative error of at most 0.015.
Values may be sent and summed in bfloat16 or wider, within the bound.
No kernel may reach another device: no remote copies, remote signals or barrier semaphores. Data moves between devices by JAX's collectives and lax.ppermute only.
A program may use at most 256 MiB of HBM per device.

```python
import math
import jax
import jax.numpy as jnp
import numpy as np
from jax import lax

D = 4608
HEADS = 32
KV_HEADS = 16
HEAD_DIM = 128
WINDOW = 4096
S_DEV = 512
SEGMENTS = 8
TOKENS = 8192
N_HEAD = 2


def draw_common(key):
    key_q, key_k = jax.random.split(key, 2)
    base_k = jnp.clip(jax.random.normal(key_k, (TOKENS, KV_HEADS, HEAD_DIM), jnp.float32), -6.0, 6.0)
    base_q = 2.5 * jnp.clip(jax.random.normal(key_q, (TOKENS, HEADS, HEAD_DIM), jnp.float32), -6.0, 6.0)
    keys_out = base_k
    queries_out = base_q
    return (queries_out.reshape(TOKENS, HEADS * HEAD_DIM), keys_out.reshape(TOKENS, KV_HEADS * HEAD_DIM))


def draw_queries(key, part):
    return draw_common(jax.random.fold_in(key, 7))[0].astype(jnp.bfloat16)


def draw_keys(key, part):
    return draw_common(jax.random.fold_in(key, 7))[1].astype(jnp.bfloat16)


def level_of(rng, dims, cuts, least, top_value):
    factor_of = 1.0
    for axis_at, shards_of in cuts:
        heights = jax.random.uniform(jax.random.fold_in(jax.random.fold_in(rng, 6), axis_at), (shards_of,), jnp.float32, least / len(cuts), top_value / len(cuts))
        factor_of = factor_of * jnp.repeat(jnp.exp(heights), dims[axis_at] // shards_of).reshape((-1,) + (1,) * (len(dims) - 1 - axis_at))
    return factor_of


def profile(amount, total, bound, skew):
    loads = [(1 << 20) // math.isqrt(standing ** skew) + 1 for standing in range(2, amount + 1)]
    rest, given = total - bound - (amount - 1), [1] * (amount - 1)
    while rest > 0:
        candidates = [i for i in range(amount - 1) if given[i] < bound]
        pool, left = sum([loads[i] for i in candidates]), rest
        for i in candidates:
            more = min(bound - given[i], max(1, left * loads[i] // pool), rest)
            given[i] = given[i] + more
            rest = rest - more
    return np.array([bound] + given)


def uneven_parts(own_key, amount, total, bound, skew):
    if amount == 2:
        one = jax.random.randint(own_key, (), max(1, total - bound), min(bound, total - 1) + 1)
        return jnp.stack([one, total - one])
    sizes = jnp.asarray(profile(amount, total, bound, skew), jnp.int32)
    twos = (amount - 1) // 2
    giver, sink = sizes[1:1 + 2 * twos:2], sizes[2:2 + 2 * twos:2]
    margin = jnp.minimum(giver - 1, bound - sink)
    shifted = jax.random.randint(jax.random.fold_in(own_key, 1), (twos,), 0, 1 << 20) % (margin + 1)
    sizes = sizes.at[1:1 + 2 * twos:2].set(giver - shifted).at[2:2 + 2 * twos:2].set(sink + shifted)
    return sizes[jax.random.permutation(jax.random.fold_in(own_key, 2), amount)]


def centred(own_key, dims, deviation, reach, pieces=(), held_as=jnp.bfloat16):
    level = level_of(own_key, dims, pieces, -0.22, 0.18) if pieces else 1.0
    result = jax.random.normal(own_key, dims, jnp.float32) * deviation * level
    return jnp.minimum(jnp.maximum(result, -reach), reach).astype(held_as)


def setup_inputs(seed: int = 0) -> dict:
    splits = jax.random.split(jax.random.key(seed), 6)
    queries = draw_queries(jax.random.fold_in(splits[5], 71), 0)
    keys = draw_keys(jax.random.fold_in(splits[5], 71), 0)
    values = centred(splits[2], (TOKENS, KV_HEADS * HEAD_DIM), 1.0, 6.0, ((0, 16), (1, 2)))
    episode = jnp.searchsorted(jnp.cumsum(uneven_parts(splits[3], SEGMENTS, TOKENS, TOKENS // 4, 1)), jnp.arange(TOKENS), side="right").astype(jnp.int32)
    out_weight = centred(splits[4], (HEADS * HEAD_DIM, D), (HEAD_DIM * HEADS // 16) ** -0.5, 0.375, ((0, 2),))
    return {"queries": queries, "keys": keys, "values": values, "episode": episode, "out_weight": out_weight}


query_scale = 1.0 / 12.0


def reference(queries, keys, values, episode, out_weight):
    ratio = HEADS // KV_HEADS
    kv_width = KV_HEADS * HEAD_DIM
    span = WINDOW + S_DEV
    padded_keys = jnp.concatenate([jnp.zeros((WINDOW, kv_width), keys.dtype), keys], axis=0)
    padded_values = jnp.concatenate([jnp.zeros((WINDOW, kv_width), values.dtype), values], axis=0)
    padded_ids = jnp.concatenate([jnp.full((WINDOW,), -1, jnp.int32), episode.astype(jnp.int32)])

    def one_block(index):
        begin = (index * S_DEV).astype(jnp.int32)
        q_block = lax.dynamic_slice_in_dim(queries, begin, S_DEV, 0).astype(jnp.float32)
        q_block = q_block.reshape(S_DEV, KV_HEADS, ratio, HEAD_DIM)
        k_block = lax.dynamic_slice_in_dim(padded_keys, begin, span, 0).astype(jnp.float32)
        k_block = k_block.reshape(span, KV_HEADS, HEAD_DIM)
        v_block = lax.dynamic_slice_in_dim(padded_values, begin, span, 0).astype(jnp.float32)
        v_block = v_block.reshape(span, KV_HEADS, HEAD_DIM)
        ids_keys = lax.dynamic_slice_in_dim(padded_ids, begin, span, 0)
        ids_query = lax.dynamic_slice_in_dim(episode.astype(jnp.int32), begin, S_DEV, 0)
        q_pos = WINDOW + jnp.arange(S_DEV, dtype=jnp.int32)
        k_pos = jnp.arange(span, dtype=jnp.int32)
        visible = (k_pos[None, :] <= q_pos[:, None]) & (k_pos[None, :] > q_pos[:, None] - WINDOW)
        visible = visible & (ids_keys[None, :] == ids_query[:, None])
        scores = jnp.einsum("sgrd,tgd->grst", q_block, k_block, precision=lax.Precision.HIGHEST) * query_scale
        scores = jnp.where(visible[None, None], scores, jnp.float32(-1e30))
        top = jnp.max(scores, axis=-1, keepdims=True)
        expd = jnp.exp(scores - top)
        weights = (expd / jnp.sum(expd, axis=-1, keepdims=True)).astype(jnp.bfloat16).astype(jnp.float32)
        mixed = jnp.einsum("grst,tgd->sgrd", weights, v_block, precision=lax.Precision.HIGHEST)
        return mixed.astype(jnp.bfloat16).reshape(S_DEV, HEADS * HEAD_DIM)

    blocks = lax.map(one_block, jnp.arange(TOKENS // S_DEV, dtype=jnp.int32))
    attended = blocks.reshape(TOKENS, HEADS * HEAD_DIM)
    width = HEADS * HEAD_DIM // N_HEAD
    total = jnp.zeros((TOKENS, D), jnp.float32)
    for group in range(N_HEAD):
        piece = jnp.dot(attended[:, group * width:(group + 1) * width], out_weight[group * width:(group + 1) * width], preferred_element_type=jnp.float32)
        piece = lax.optimization_barrier(piece.astype(jnp.bfloat16))
        total = total + piece.astype(jnp.float32)
    return total.astype(jnp.bfloat16)
```

```python
import math

import jax
import jax.numpy as jnp
from jax import lax
from jax.experimental import pallas as pl
from jax.experimental.pallas import tpu as pltpu
from jax.sharding import PartitionSpec as P

HEAD_DIM = 128
WINDOW = 4096

SCORE_SCALE = math.log2(math.e) / 12.0
HIDDEN = -1e30


def plan(rows, kv_heads, seq_size, tokens):
    reach = min(WINDOW, tokens // 4)
    group = math.gcd(kv_heads, seq_size)
    group &= -group
    while group > 1 and group * rows > reach:
        group //= 2
    before = -(-(reach - 1) // (group * rows))
    back = -(-(reach - 1) // rows)
    return group, before, back


def attend_kernel(group, before, back, ratio, rows, meta, qid, kid, *refs):
    n_kv = group * (before + 1)
    kv_in, refs = refs[:n_kv], refs[n_kv:]
    q_in, refs = refs[:group], refs[group:]
    outs, refs = refs[:group], refs[group:]
    k_all, v_all, q_all, scores, top, acc, o_all, sem_in, sem_out = refs
    me = meta[0]
    base = before * group
    copies = []
    for n, ref in enumerate(kv_in):
        slot = (n // group) * group + (me ^ (n % group))
        copies.append(pltpu.make_async_copy(ref.at[:, :HEAD_DIM], k_all.at[slot], sem_in.at[3 * n]))
        copies.append(
            pltpu.make_async_copy(
                ref.at[:, HEAD_DIM:], v_all.at[slot, :, pl.ds(0, HEAD_DIM)], sem_in.at[3 * n + 1]
            )
        )
    for n, ref in enumerate(q_in):
        copies.append(pltpu.make_async_copy(ref, q_all.at[n], sem_in.at[3 * n + 2]))
    for copy in copies:
        copy.start()
    v_all[:, :, HEAD_DIM:] = jnp.ones((n_kv, rows, HEAD_DIM), jnp.bfloat16)
    for copy in copies:
        copy.wait()

    def one_block(r, carry):
        at = base + (me ^ r)
        first = meta[1 + r]
        full = meta[1 + group + r]
        top[...] = jnp.full(top.shape, HIDDEN, jnp.float32)
        acc[...] = jnp.zeros(acc.shape, jnp.float32)

        def score(j, masked, diagonal):
            k = k_all[j]
            if masked:
                own = jnp.concatenate([qid[me ^ r]] * (rows // HEAD_DIM), axis=1)
                seen = own == kid[j]
                q_pos = lax.broadcasted_iota(jnp.int32, (rows, rows), 0)
                k_pos = lax.broadcasted_iota(jnp.int32, (rows, rows), 1)
                if diagonal:
                    seen = seen & (k_pos <= q_pos)
                if n_kv * rows > WINDOW or diagonal:
                    seen = seen & (k_pos - q_pos > (at - j) * rows - WINDOW)
            for h in range(ratio):
                q = q_all[r, :, h * HEAD_DIM : (h + 1) * HEAD_DIM]
                s = lax.dot_general(q, k, (((1,), (1,)), ((), ())), preferred_element_type=jnp.float32)
                if masked:
                    s = jnp.where(seen, s, HIDDEN)
                scores[at - j, h] = s
                m = top[h]
                for part in range(rows // HEAD_DIM):
                    m = jnp.maximum(m, s[:, part * HEAD_DIM : (part + 1) * HEAD_DIM])
                top[h] = m

        def masked_step(j, c):
            score(j, True, False)
            return c

        def full_step(j, c):
            score(j, False, False)
            return c

        lax.fori_loop(first, full, masked_step, 0)
        lax.fori_loop(full, at, full_step, 0)
        score(at, True, True)
        for h in range(ratio):
            m = jnp.max(top[h], axis=1, keepdims=True) * SCORE_SCALE
            top[h] = jnp.broadcast_to(m, (rows, HEAD_DIM))

        def mix_step(j, c):
            for h in range(ratio):
                m = jnp.concatenate([top[h]] * (rows // HEAD_DIM), axis=1)
                p = jnp.exp2(scores[at - j, h] * SCORE_SCALE - m).astype(jnp.bfloat16)
                acc[h] += jnp.dot(p, v_all[j], preferred_element_type=jnp.float32)
            return c

        lax.fori_loop(first, at + 1, mix_step, 0)
        for h in range(ratio):
            o = acc[h, :, :HEAD_DIM] / acc[h, :, HEAD_DIM:]
            o_all[r, :, h * HEAD_DIM : (h + 1) * HEAD_DIM] = o.astype(jnp.bfloat16)
        for n in range(group):

            @pl.when(r == n)
            def _():
                pltpu.make_async_copy(o_all.at[n], outs[n], sem_out.at[n]).start()

        return carry

    lax.fori_loop(0, group, one_block, 0)
    for n in range(group):
        pltpu.make_async_copy(o_all.at[n], outs[n], sem_out.at[n]).wait()


def attend(meta, qid, kid, kv, q, group, before, back):
    rows, width = q[0].shape
    ratio = width // HEAD_DIM
    n_kv = len(kv)
    hbm = pl.BlockSpec(memory_space=pl.ANY)
    vmem = pl.BlockSpec(memory_space=pltpu.VMEM)
    return pl.pallas_call(
        lambda *refs: attend_kernel(group, before, back, ratio, rows, *refs),
        out_shape=[jax.ShapeDtypeStruct((rows, width), jnp.bfloat16)] * group,
        in_specs=[pl.BlockSpec(memory_space=pltpu.SMEM), vmem, vmem] + [hbm] * (n_kv + group),
        out_specs=[hbm] * group,
        scratch_shapes=[
            pltpu.VMEM((n_kv, rows, HEAD_DIM), jnp.bfloat16),
            pltpu.VMEM((n_kv, rows, 2 * HEAD_DIM), jnp.bfloat16),
            pltpu.VMEM((group, rows, width), jnp.bfloat16),
            pltpu.VMEM((back + 1, ratio, rows, rows), jnp.float32),
            pltpu.VMEM((ratio, rows, HEAD_DIM), jnp.float32),
            pltpu.VMEM((ratio, rows, 2 * HEAD_DIM), jnp.float32),
            pltpu.VMEM((group, rows, width), jnp.bfloat16),
            pltpu.SemaphoreType.DMA((3 * n_kv,)),
            pltpu.SemaphoreType.DMA((group,)),
        ],
    )(meta, qid, kid, *kv, *q)


def project(scalars, mixed, weight, chunk, columns, addend, dtype):
    group = len(mixed)
    rows, width = mixed[0].shape
    tile = max(t for t in range(128, 769, 128) if columns % t == 0)
    steps = columns // tile

    def kernel(info, *refs):
        pieces, w, out = refs[:group], refs[group], refs[-1]
        total = refs[group + 1][...] if addend is not None else None
        for r in range(group):
            start = pl.multiple_of((info[0] ^ r) * width, width)
            part = jnp.dot(pieces[r][...], w[pl.ds(start, width), :], preferred_element_type=jnp.float32)
            total = part if total is None else total + part
        out[...] = total.astype(dtype)

    whole = pl.BlockSpec((rows, width), lambda n, info: (0, 0))
    tiled = pl.BlockSpec((rows, tile), lambda n, info: (0, n))
    w_spec = pl.BlockSpec((group * width, tile), lambda n, info: (chunk, info[1] * steps + n))
    extra = [] if addend is None else [addend]
    return pl.pallas_call(
        kernel,
        out_shape=jax.ShapeDtypeStruct((rows, columns), dtype),
        grid_spec=pltpu.PrefetchScalarGridSpec(
            num_scalar_prefetch=1,
            grid=(steps,),
            in_specs=[whole] * group + [w_spec] + [tiled] * len(extra),
            out_specs=tiled,
        ),
    )(scalars, *mixed, weight, *extra)


def body(queries, keys, values, episode, out_weight):
    rows = queries.shape[0]
    tokens = episode.shape[0]
    seq_size = lax.axis_size("seq")
    head_size = lax.axis_size("head")
    kv_heads = keys.shape[1] // HEAD_DIM
    ratio = queries.shape[1] // keys.shape[1]
    group, before, back = plan(rows, kv_heads, seq_size, tokens)
    chunks = kv_heads // group
    me = lax.axis_index("seq") % group
    mine = lax.axis_index("seq") // group
    head = lax.axis_index("head")
    n_kv = (before + 1) * group

    def swap(value, r):
        return lax.ppermute(value, "seq", [(s, s ^ r) for s in range(seq_size)]) if r else value

    def upward(value, p):
        step = p * group
        return lax.ppermute(value, "seq", [(s, s + step) for s in range(seq_size - step)])

    def columns_of(value, at, heads):
        return lax.dynamic_slice_in_dim(value, at * heads * HEAD_DIM, heads * HEAD_DIM, 1)

    own_kv, far_kv, own_q = [], [], []
    for c in range(chunks):
        pieces = []
        for r in range(group):
            at = c * group + (me ^ r)
            pieces.append(jnp.concatenate([columns_of(keys, at, 1), columns_of(values, at, 1)], axis=1))
        own_kv.append([swap(piece, r) for r, piece in enumerate(pieces)])
    for c in range(chunks):
        far_kv.append([upward(piece, p) for p in range(before, 0, -1) for piece in own_kv[c]])
    for c in range(chunks):
        own_q.append([swap(columns_of(queries, c * group + (me ^ r), ratio), r) for r in range(group)])

    padded = jnp.concatenate([jnp.full((before * group * rows,), -1, jnp.int32), episode])
    ids = lax.dynamic_slice_in_dim(padded, mine * group * rows, n_kv * rows, 0).reshape(n_kv, rows)
    first_id, last_id = ids[:, 0], ids[:, -1]
    at = before * group + (me ^ jnp.arange(group, dtype=jnp.int32))
    first = jnp.sum(last_id[None, :] < jnp.take(first_id, at)[:, None], axis=1, dtype=jnp.int32)
    first = jnp.clip(first, at - back, at)
    full = jnp.sum(first_id[None, :] < jnp.take(last_id, at)[:, None], axis=1, dtype=jnp.int32)
    full = jnp.maximum(full, at + 1 - WINDOW // rows)
    full = jnp.clip(full, first, at)
    meta = jnp.concatenate([me[None].astype(jnp.int32), first, full])
    qid = jnp.broadcast_to(ids[before * group :, :, None], (group, rows, HEAD_DIM))
    kid = ids[:, None, :]

    partial = [None] * head_size
    columns = out_weight.shape[1] // head_size
    for c in range(chunks):
        mixed = attend(meta, qid, kid, far_kv[c] + own_kv[c], own_q[c], group, before, back)
        mixed = [swap(piece, r) for r, piece in enumerate(mixed)]
        dtype = jnp.float32 if c + 1 < chunks else jnp.bfloat16
        for d in list(range(1, head_size)) + [0]:
            scalars = jnp.stack([me, (head + d) % head_size]).astype(jnp.int32)
            partial[d] = project(scalars, mixed, out_weight, c, columns, partial[d], dtype)
    total = partial[0].astype(jnp.float32)
    for d in range(1, head_size):
        ring = [(s, (s + d) % head_size) for s in range(head_size)]
        total = total + lax.ppermute(partial[d], "head", ring).astype(jnp.float32)
    return total.astype(jnp.bfloat16)


def solution(mesh):
    placed = (P("seq", "head"), P("seq", "head"), P("seq", "head"), P(), P("head", None))
    return jax.shard_map(
        body, mesh=mesh, in_specs=placed, out_specs=P("seq", "head"), check_vma=False
    )
```

```python
import math

import jax
import jax.numpy as jnp
from jax import lax
from jax.experimental import pallas as pl
from jax.experimental.pallas import tpu as pltpu
from jax.sharding import PartitionSpec as P


HEAD_DIM = 128
WINDOW = 4096

SCORE_SCALE = math.log2(math.e) / 12.0
HIDDEN = -1e30


def plan(rows, kv_heads, seq_size, tokens):
    reach = min(WINDOW, tokens // 4)
    group = math.gcd(kv_heads, seq_size)
    group &= -group
    while group > 1 and group * rows > reach:
        group //= 2
    before = -(-(reach - 1) // (group * rows))
    back = -(-(reach - 1) // rows)
    return group, before, back


def attend_kernel(chunk, group, before, ratio, rows, meta, qid, kid, *refs):
    n_kv = group * (before + 1)
    far, refs = refs[: 2 * before], refs[2 * before :]
    near, refs = refs[:group], refs[group:]
    q_in, refs = refs[:group], refs[group:]
    outs, refs = refs[:group], refs[group:]
    k_all, v_all, q_all, scores, top, acc = refs
    me = meta[0]
    base = before * group

    def place(ref, row, column, slot):
        at = slice(row, row + rows)
        k_all[slot] = ref[at, column : column + HEAD_DIM]
        v_all[slot, :, :HEAD_DIM] = ref[at, column + HEAD_DIM : column + 2 * HEAD_DIM]

    for p in range(before):
        place(far[2 * p], 0, chunk * 2 * HEAD_DIM, p * group + me)
        for r in range(1, group):
            place(far[2 * p + 1], (r - 1) * rows, 0, p * group + (me ^ r))
    for r in range(group):
        place(near[r], 0, 0, base + (me ^ r))
        q_all[r] = q_in[r][...]
    v_all[:, :, HEAD_DIM:] = jnp.ones((n_kv, rows, HEAD_DIM), jnp.bfloat16)

    def one_block(r, carry):
        at = base + (me ^ r)
        first = meta[1 + r]
        full = meta[1 + group + r]
        top[...] = jnp.full(top.shape, HIDDEN, jnp.float32)
        acc[...] = jnp.zeros(acc.shape, jnp.float32)

        def score(j, masked, diagonal):
            k = k_all[j]
            if masked:
                own = jnp.concatenate([qid[me ^ r]] * (rows // HEAD_DIM), axis=1)
                seen = own == kid[j]
                q_pos = lax.broadcasted_iota(jnp.int32, (rows, rows), 0)
                k_pos = lax.broadcasted_iota(jnp.int32, (rows, rows), 1)
                if diagonal:
                    seen = seen & (k_pos <= q_pos)
                if n_kv * rows > WINDOW or diagonal:
                    seen = seen & (k_pos - q_pos > (at - j) * rows - WINDOW)
            for h in range(ratio):
                q = q_all[r, :, h * HEAD_DIM : (h + 1) * HEAD_DIM]
                s = lax.dot_general(q, k, (((1,), (1,)), ((), ())), preferred_element_type=jnp.float32)
                if masked:
                    s = jnp.where(seen, s, HIDDEN)
                scores[at - j, h] = s
                m = top[h]
                for part in range(rows // HEAD_DIM):
                    m = jnp.maximum(m, s[:, part * HEAD_DIM : (part + 1) * HEAD_DIM])
                top[h] = m

        def masked_step(j, c):
            score(j, True, False)
            return c

        def full_step(j, c):
            score(j, False, False)
            return c

        lax.fori_loop(first, full, masked_step, 0)
        lax.fori_loop(full, at, full_step, 0)
        score(at, True, True)
        for h in range(ratio):
            m = jnp.max(top[h], axis=1, keepdims=True) * SCORE_SCALE
            top[h] = jnp.broadcast_to(m, (rows, HEAD_DIM))

        def mix_step(j, c):
            for h in range(ratio):
                m = jnp.concatenate([top[h]] * (rows // HEAD_DIM), axis=1)
                p = jnp.exp2(scores[at - j, h] * SCORE_SCALE - m).astype(jnp.bfloat16)
                acc[h] += jnp.dot(p, v_all[j], preferred_element_type=jnp.float32)
            return c

        lax.fori_loop(first, at + 1, mix_step, 0)
        for h in range(ratio):
            o = (acc[h, :, :HEAD_DIM] / acc[h, :, HEAD_DIM:]).astype(jnp.bfloat16)
            for n in range(group):

                @pl.when(r == n)
                def _():
                    outs[n][:, h * HEAD_DIM : (h + 1) * HEAD_DIM] = o

        return carry

    lax.fori_loop(0, group, one_block, 0)


def attend(meta, qid, kid, far, near, q, chunk, group, before, back):
    rows = near[0].shape[0]
    width = q[0].shape[1]
    ratio = width // HEAD_DIM
    n_kv = (before + 1) * group
    vmem = pl.BlockSpec(memory_space=pltpu.VMEM)
    return pl.pallas_call(
        lambda *refs: attend_kernel(chunk, group, before, ratio, rows, *refs),
        out_shape=[jax.ShapeDtypeStruct((rows, width), jnp.bfloat16)] * group,
        in_specs=[pl.BlockSpec(memory_space=pltpu.SMEM)] + [vmem] * (2 + len(far) + len(near) + group),
        out_specs=[vmem] * group,
        scratch_shapes=[
            pltpu.VMEM((n_kv, rows, HEAD_DIM), jnp.bfloat16),
            pltpu.VMEM((n_kv, rows, 2 * HEAD_DIM), jnp.bfloat16),
            pltpu.VMEM((group, rows, width), jnp.bfloat16),
            pltpu.VMEM((back + 1, ratio, rows, rows), jnp.float32),
            pltpu.VMEM((ratio, rows, HEAD_DIM), jnp.float32),
            pltpu.VMEM((ratio, rows, 2 * HEAD_DIM), jnp.float32),
        ],
        compiler_params=pltpu.CompilerParams(vmem_limit_bytes=40 << 20),
    )(meta, qid, kid, *far, *near, *q)


def project(me, targets, left, weight, chunk, columns, addends, dtype):
    group = len(left)
    assembled = group == 1
    rows = left[0].shape[-2]
    group, width = left[0].shape[::2] if assembled else (group, left[0].shape[1])
    tile = max(t for t in range(128, 769, 128) if columns % t == 0)
    per = columns // tile
    count = len(targets)
    steps = count * per

    def kernel(info, *refs):
        pieces, refs = refs[: len(left)], refs[len(left) :]
        w, refs = refs[0], refs[1:]
        added, refs = refs[: len(addends)], refs[len(addends) :]
        outs, (w_all, sem) = refs[:-2], refs[-2:]
        lhs = pieces[0] if assembled else outs[-1]

        def fetch(t, n):
            at = pl.ds(pl.multiple_of(info[1 + t] * columns + n * tile, 128), tile)
            row = chunk * group * width
            slot = t * per + n
            return pltpu.make_async_copy(w.at[pl.ds(row, group * width), at], w_all.at[slot], sem.at[slot])

        for t in range(count):
            for n in range(per):
                fetch(t, n).start()
        if not assembled:
            for r in range(group):
                lhs[info[0] ^ r] = pieces[r][...]
        for t in range(count):

            def step(n, carry):
                fetch(t, n).wait()
                here = pl.ds(pl.multiple_of(n * tile, 128), tile)
                wide = jnp.concatenate([lhs[u] for u in range(group)], axis=1)
                total = jnp.dot(wide, w_all[t * per + n], preferred_element_type=jnp.float32)
                if addends:
                    total = total + added[t][:, here]
                outs[t][:, here] = total.astype(dtype)
                return carry

            lax.fori_loop(0, per, step, 0)

    vmem = pl.BlockSpec(memory_space=pltpu.VMEM)
    hbm = pl.BlockSpec(memory_space=pltpu.HBM)
    shapes = [jax.ShapeDtypeStruct((rows, columns), dtype)] * count
    if not assembled:
        shapes.append(jax.ShapeDtypeStruct((group, rows, width), jnp.bfloat16))
    return pl.pallas_call(
        kernel,
        out_shape=shapes,
        in_specs=[pl.BlockSpec(memory_space=pltpu.SMEM)] + [vmem] * len(left) + [hbm] + [vmem] * len(addends),
        out_specs=[vmem] * len(shapes),
        scratch_shapes=[
            pltpu.VMEM((steps, group * width, tile), jnp.bfloat16),
            pltpu.SemaphoreType.DMA((steps,)),
        ],
        compiler_params=pltpu.CompilerParams(vmem_limit_bytes=40 << 20),
    )(jnp.stack([me, *targets]).astype(jnp.int32), *left, weight, *addends)


def add_up(parts):
    rows, columns = parts[0].shape
    tile = max(t for t in range(8, 129, 8) if rows % t == 0)

    def kernel(*refs):
        out, held, sem = refs[-3:]

        def moved(n):
            at = pl.ds(pl.multiple_of(n * tile, 8), tile)
            return pltpu.make_async_copy(held.at[at], out.at[at], sem.at[n])

        def step(n, carry):
            at = pl.ds(pl.multiple_of(n * tile, 8), tile)
            total = refs[0][at].astype(jnp.float32)
            for ref in refs[1:-3]:
                total = total + ref[at].astype(jnp.float32)
            held[at] = total.astype(jnp.bfloat16)
            moved(n).start()
            return carry

        lax.fori_loop(0, rows // tile, step, 0)
        for n in range(rows // tile):
            moved(n).wait()

    return pl.pallas_call(
        kernel,
        out_shape=jax.ShapeDtypeStruct((rows, columns), jnp.bfloat16),
        in_specs=[pl.BlockSpec(memory_space=pltpu.VMEM)] * len(parts),
        out_specs=pl.BlockSpec(memory_space=pltpu.HBM),
        scratch_shapes=[
            pltpu.VMEM((rows, columns), jnp.bfloat16),
            pltpu.SemaphoreType.DMA((rows // tile,)),
        ],
        compiler_params=pltpu.CompilerParams(vmem_limit_bytes=12 << 20),
    )(*parts)


def body(queries, keys, values, episode, out_weight):
    rows = queries.shape[0]
    tokens = episode.shape[0]
    seq_size = lax.axis_size("seq")
    head_size = lax.axis_size("head")
    kv_heads = keys.shape[1] // HEAD_DIM
    ratio = queries.shape[1] // keys.shape[1]
    group, before, back = plan(rows, kv_heads, seq_size, tokens)
    chunks = kv_heads // group
    me = lax.axis_index("seq") % group
    mine = lax.axis_index("seq") // group
    head = lax.axis_index("head")
    n_kv = (before + 1) * group

    def swap(value, r):
        if not r:
            return value
        return lax.ppermute(value, "seq", [(s, s ^ r) for s in range(seq_size)])

    def upward(value, p):
        step = p * group
        return lax.ppermute(value, "seq", [(s, s + step) for s in range(seq_size - step)])

    def columns_of(value, at, heads):
        return lax.dynamic_slice_in_dim(value, at * heads * HEAD_DIM, heads * HEAD_DIM, 1)

    def pair_of(c, r):
        at = c * group + (me ^ r)
        return [columns_of(keys, at, 1), columns_of(values, at, 1)]

    near = [
        [swap(jnp.concatenate(pair_of(c, r), axis=1), r) for r in range(group)]
        for c in range(chunks)
    ]
    own = jnp.concatenate([piece for c in range(chunks) for piece in pair_of(c, 0)], axis=1)
    far_own = [upward(own, p) for p in range(before, 0, -1)]
    own_q = [
        [swap(columns_of(queries, c * group + (me ^ r), ratio), r) for r in range(group)]
        for c in range(chunks)
    ]
    far = []
    for c in range(chunks):
        rest = jnp.concatenate(near[c][1:], axis=0)
        moved = [upward(rest, p) for p in range(before, 0, -1)]
        far.append([piece for pair in zip(far_own, moved) for piece in pair])

    padded = jnp.concatenate([jnp.full((before * group * rows,), -1, jnp.int32), episode])
    ids = lax.dynamic_slice_in_dim(padded, mine * group * rows, n_kv * rows, 0).reshape(n_kv, rows)
    first_id, last_id = ids[:, 0], ids[:, -1]
    at = before * group + (me ^ jnp.arange(group, dtype=jnp.int32))
    first = jnp.sum(last_id[None, :] < jnp.take(first_id, at)[:, None], axis=1, dtype=jnp.int32)
    first = jnp.clip(first, at - back, at)
    full = jnp.sum(first_id[None, :] < jnp.take(last_id, at)[:, None], axis=1, dtype=jnp.int32)
    full = jnp.maximum(full, at + 1 - WINDOW // rows)
    full = jnp.clip(full, first, at)
    meta = jnp.concatenate([me[None].astype(jnp.int32), first, full])
    qid = jnp.broadcast_to(ids[before * group :, :, None], (group, rows, HEAD_DIM))
    kid = ids[:, None, :]

    columns = out_weight.shape[1] // head_size
    targets = [(head + d) % head_size for d in list(range(1, head_size)) + [0]]
    sums = []
    for c in range(chunks):
        mixed = attend(meta, qid, kid, far[c], near[c], own_q[c], c, group, before, back)
        mixed = [swap(piece, r) for r, piece in enumerate(mixed)]
        if c + 1 < chunks:
            *sums, _ = project(me, targets, mixed, out_weight, c, columns, sums, jnp.float32)
    *sent, mixed = project(me, targets[:-1], mixed, out_weight, c, columns, sums[:-1], jnp.bfloat16)
    (kept,) = project(me, targets[-1:], [mixed], out_weight, c, columns, sums[-1:], jnp.bfloat16)
    for d in range(1, head_size):
        ring = [(s, (s + d) % head_size) for s in range(head_size)]
        sent[d - 1] = lax.ppermute(sent[d - 1], "head", ring)
    return add_up([kept, *sent])


def solution(mesh):
    placed = (P("seq", "head"), P("seq", "head"), P("seq", "head"), P(), P("head", None))
    return jax.shard_map(
        body, mesh=mesh, in_specs=placed, out_specs=P("seq", "head"), check_vma=False
    )
```

```python
import math

import jax
import jax.numpy as jnp
from jax import lax
from jax.experimental import pallas as pl
from jax.experimental.pallas import tpu as pltpu
from jax.sharding import PartitionSpec as P


HEAD_DIM = 128
WINDOW = 4096

SCORE_SCALE = math.log2(math.e) / 12.0
HIDDEN = -1e30
ATTEND_ROOM = 16 << 20
PROJECT_ROOM = 26 << 20
SPLIT = False


def plan(rows, kv_heads, seq_size, tokens):
    reach = min(WINDOW, tokens // 4)
    group = math.gcd(kv_heads, seq_size)
    group &= -group
    while group > 1 and group * rows > reach:
        group //= 2
    before = -(-(reach - 1) // (group * rows))
    back = -(-(reach - 1) // rows)
    return group, before, back


def attend_kernel(chunk, group, before, ratio, rows, start, stride, count, meta, qid, kid, *refs):
    n_kv = group * (before + 1)
    far, refs = refs[: 2 * before], refs[2 * before :]
    near, refs = refs[:group], refs[group:]
    q_in, refs = refs[:count], refs[count:]
    outs, refs = refs[:count], refs[count:]
    k_all, v_all, q_all, scores, top, acc = refs
    me = meta[0]
    base = before * group
    cut = rows // 2 if rows % (2 * HEAD_DIM) == 0 else rows

    def place(ref, row, column, slot):
        at = slice(row, row + rows)
        k_all[slot] = ref[at, column : column + HEAD_DIM]
        v_all[slot, :, :HEAD_DIM] = ref[at, column + HEAD_DIM : column + 2 * HEAD_DIM]

    own_column = chunk * 2 * HEAD_DIM
    for p in range(before):
        place(far[2 * p], 0, own_column, p * group + me)
        for r in range(1, group):
            place(far[2 * p + 1], (r - 1) * rows, 0, p * group + (me ^ r))
    for r in range(group):
        place(near[r], 0, 0 if r else own_column, base + (me ^ r))
    for n in range(count):
        q_all[n] = q_in[n][...]
    v_all[:, :, HEAD_DIM:] = jnp.ones((n_kv, rows, HEAD_DIM), jnp.bfloat16)

    def folded(s):
        parts = [s[:, n : n + HEAD_DIM] for n in range(0, s.shape[1], HEAD_DIM)]
        while len(parts) > 1:
            parts = [jnp.maximum(*parts[n : n + 2]) if n + 1 < len(parts) else parts[n] for n in range(0, len(parts), 2)]
        return parts[0]

    def one_block(n, carry):
        r = start + stride * n
        at = base + (me ^ r)
        first = meta[1 + r]
        full = meta[1 + group + r]

        def product(h, low, high, keys):
            q = q_all[n, low:high, h * HEAD_DIM : (h + 1) * HEAD_DIM]
            return lax.dot_general(q, keys, (((1,), (1,)), ((), ())), preferred_element_type=jnp.float32)

        def positions(low, high, wide):
            shape = (high - low, wide)
            q_pos = lax.broadcasted_iota(jnp.int32, shape, 0) + low
            return q_pos, lax.broadcasted_iota(jnp.int32, shape, 1)

        def same_episode(j, low, high, wide):
            own = jnp.concatenate([qid[me ^ r, low:high]] * (wide // HEAD_DIM), axis=1)
            return own == kid[j, :, :wide]

        for low in range(0, rows, cut):
            high = low + cut
            q_pos, k_pos = positions(low, high, high)
            seen = same_episode(at, low, high, high) & (k_pos <= q_pos)
            if rows > WINDOW:
                seen = seen & (k_pos - q_pos > -WINDOW)
            for h in range(ratio):
                s = jnp.where(seen, product(h, low, high, k_all[at, :high]), HIDDEN)
                scores[0, h, low:high, :high] = s
                top[h, low:high] = folded(s)

        def score(j, masked):
            keys = k_all[j]
            if masked:
                seen = same_episode(j, 0, rows, rows)
                if n_kv * rows > WINDOW:
                    q_pos, k_pos = positions(0, rows, rows)
                    seen = seen & (k_pos - q_pos > (at - j) * rows - WINDOW)
            for h in range(ratio):
                s = product(h, 0, rows, keys)
                if masked:
                    s = jnp.where(seen, s, HIDDEN)
                scores[at - j, h] = s
                top[h] = jnp.maximum(top[h], folded(s))

        def masked_step(j, c):
            score(j, True)
            return c

        def full_step(j, c):
            score(j, False)
            return c

        lax.fori_loop(first, full, masked_step, 0)
        lax.fori_loop(full, at, full_step, 0)
        for h in range(ratio):
            m = jnp.max(top[h], axis=1, keepdims=True) * SCORE_SCALE
            top[h] = jnp.broadcast_to(m, (rows, HEAD_DIM))

        def weighted(j, h, low, high, wide):
            m = jnp.concatenate([top[h, low:high]] * (wide // HEAD_DIM), axis=1)
            p = jnp.exp2(scores[at - j, h, low:high, :wide] * SCORE_SCALE - m).astype(jnp.bfloat16)
            return jnp.dot(p, v_all[j, :wide], preferred_element_type=jnp.float32)

        for h in range(ratio):
            for low in range(0, rows, cut):
                acc[h, low : low + cut] = weighted(at, h, low, low + cut, low + cut)

        def mix_step(j, c):
            for h in range(ratio):
                acc[h] += weighted(j, h, 0, rows, rows)
            return c

        lax.fori_loop(first, at, mix_step, 0)
        for h in range(ratio):
            o = (acc[h, :, :HEAD_DIM] / acc[h, :, HEAD_DIM:]).astype(jnp.bfloat16)
            for k in range(count):

                @pl.when(n == k)
                def _():
                    outs[k][:, h * HEAD_DIM : (h + 1) * HEAD_DIM] = o

        return carry

    lax.fori_loop(0, count, one_block, 0)


def attend(meta, qid, kid, far, near, q, chunk, group, before, back, start, stride):
    rows, width = q[0].shape
    ratio = width // HEAD_DIM
    n_kv = (before + 1) * group
    count = len(q)
    vmem = pl.BlockSpec(memory_space=pltpu.VMEM)
    tiles = (back + 1) * ratio * rows * rows * 4
    return pl.pallas_call(
        lambda *refs: attend_kernel(chunk, group, before, ratio, rows, start, stride, count, *refs),
        out_shape=[jax.ShapeDtypeStruct((rows, width), jnp.bfloat16)] * count,
        in_specs=[pl.BlockSpec(memory_space=pltpu.SMEM)] + [vmem] * (2 + len(far) + len(near) + count),
        out_specs=[vmem] * count,
        scratch_shapes=[
            pltpu.VMEM((n_kv, rows, HEAD_DIM), jnp.bfloat16),
            pltpu.VMEM((n_kv, rows, 2 * HEAD_DIM), jnp.bfloat16),
            pltpu.VMEM((count, rows, width), jnp.bfloat16),
            pltpu.VMEM((back + 1, ratio, rows, rows), jnp.float32),
            pltpu.VMEM((ratio, rows, HEAD_DIM), jnp.float32),
            pltpu.VMEM((ratio, rows, 2 * HEAD_DIM), jnp.float32),
        ],
        compiler_params=pltpu.CompilerParams(vmem_limit_bytes=tiles + ATTEND_ROOM),
    )(meta, qid, kid, *far, *near, *q)


def project(me, targets, left, weight, chunk, columns, addends, dtype, ahead=None, ready=()):
    assembled = len(left) == 1
    group, rows, width = left[0].shape if assembled else (len(left), *left[0].shape)
    depth = group * width
    tile = max(t for t in range(128, 769, 128) if columns % t == 0)
    per = columns // tile
    count = len(targets)
    steps = count * per
    more = count if ahead is not None else 0

    def kernel(info, *refs):
        pieces, refs = refs[: len(left)], refs[len(left) :]
        w, refs = refs[: max(1, len(ready))], refs[max(1, len(ready)) :]
        added, refs = refs[: len(addends)], refs[len(addends) :]
        outs, (w_all, sem, sem_ahead) = refs[:-3], refs[-3:]
        lhs = pieces[0] if assembled else outs[count]

        def fetch(t, n):
            at = pl.ds(pl.multiple_of(info[1 + t] * columns + n * tile, 128), tile)
            slot = t * per + n
            source = w[0].at[pl.ds(chunk * depth, depth), at]
            return pltpu.make_async_copy(source, w_all.at[slot], sem.at[slot])

        def fetch_ahead(t):
            at = pl.ds(pl.multiple_of(info[1 + t] * columns, 128), columns)
            source = w[0].at[pl.ds(ahead * depth, depth), at]
            return pltpu.make_async_copy(source, outs[len(outs) - more + t], sem_ahead.at[t])

        if not ready:
            for t in range(count):
                for n in range(per):
                    fetch(t, n).start()
        for t in range(more):
            fetch_ahead(t).start()
        if not assembled:
            for r in range(group):
                lhs[info[0] ^ r] = pieces[r][...]
        for t in range(count):

            def step(n, carry):
                here = pl.ds(pl.multiple_of(n * tile, 128), tile)
                if ready:
                    w_tile = w[t][:, here]
                else:
                    fetch(t, n).wait()
                    w_tile = w_all[t * per + n]
                wide = jnp.concatenate([lhs[u] for u in range(group)], axis=1)
                total = jnp.dot(wide, w_tile, preferred_element_type=jnp.float32)
                if addends:
                    total = total + added[t][:, here]
                outs[t][:, here] = total.astype(dtype)
                return carry

            lax.fori_loop(0, per, step, 0)
        for t in range(more):
            fetch_ahead(t).wait()

    vmem = pl.BlockSpec(memory_space=pltpu.VMEM)
    hbm = pl.BlockSpec(memory_space=pltpu.HBM)
    shapes = [jax.ShapeDtypeStruct((rows, columns), dtype)] * count
    if not assembled:
        shapes.append(jax.ShapeDtypeStruct((group, rows, width), jnp.bfloat16))
    shapes += [jax.ShapeDtypeStruct((depth, columns), jnp.bfloat16)] * more
    return pl.pallas_call(
        kernel,
        out_shape=shapes,
        in_specs=[pl.BlockSpec(memory_space=pltpu.SMEM)]
        + [vmem] * len(left)
        + ([vmem] * len(ready) or [hbm])
        + [vmem] * len(addends),
        out_specs=[vmem] * len(shapes),
        scratch_shapes=[
            pltpu.VMEM((1, 16, 128) if ready else (steps, depth, tile), jnp.bfloat16),
            pltpu.SemaphoreType.DMA((steps,)),
            pltpu.SemaphoreType.DMA((max(1, more),)),
        ],
        compiler_params=pltpu.CompilerParams(vmem_limit_bytes=PROJECT_ROOM),
    )(jnp.stack([me, *targets]).astype(jnp.int32), *left, *(ready or [weight]), *addends)


def add_up(parts):
    rows, columns = parts[0].shape
    tile = max(t for t in range(8, 129, 8) if rows % t == 0)

    def kernel(*refs):
        out, held, sem = refs[-3:]

        def moved(n):
            at = pl.ds(pl.multiple_of(n * tile, 8), tile)
            return pltpu.make_async_copy(held.at[at], out.at[at], sem.at[n])

        def step(n, carry):
            at = pl.ds(pl.multiple_of(n * tile, 8), tile)
            total = refs[0][at].astype(jnp.float32)
            for ref in refs[1:-3]:
                total = total + ref[at].astype(jnp.float32)
            held[at] = total.astype(jnp.bfloat16)
            moved(n).start()
            return carry

        lax.fori_loop(0, rows // tile, step, 0)
        for n in range(rows // tile):
            moved(n).wait()

    return pl.pallas_call(
        kernel,
        out_shape=jax.ShapeDtypeStruct((rows, columns), jnp.bfloat16),
        in_specs=[pl.BlockSpec(memory_space=pltpu.VMEM)] * len(parts),
        out_specs=pl.BlockSpec(memory_space=pltpu.HBM),
        scratch_shapes=[
            pltpu.VMEM((rows, columns), jnp.bfloat16),
            pltpu.SemaphoreType.DMA((rows // tile,)),
        ],
        compiler_params=pltpu.CompilerParams(vmem_limit_bytes=12 << 20),
    )(*parts)


def body(queries, keys, values, episode, out_weight):
    rows = queries.shape[0]
    tokens = episode.shape[0]
    seq_size = lax.axis_size("seq")
    head_size = lax.axis_size("head")
    kv_heads = keys.shape[1] // HEAD_DIM
    ratio = queries.shape[1] // keys.shape[1]
    group, before, back = plan(rows, kv_heads, seq_size, tokens)
    chunks = kv_heads // group
    me = lax.axis_index("seq") % group
    mine = lax.axis_index("seq") // group
    head = lax.axis_index("head")
    n_kv = (before + 1) * group

    def swap(value, r):
        if not r:
            return value
        return lax.ppermute(value, "seq", [(s, s ^ r) for s in range(seq_size)])

    def upward(value, p):
        step = p * group
        return lax.ppermute(value, "seq", [(s, s + step) for s in range(seq_size - step)])

    def columns_of(value, at, heads):
        return lax.dynamic_slice_in_dim(value, at * heads * HEAD_DIM, heads * HEAD_DIM, 1)

    def pair_of(c, r):
        at = c * group + (me ^ r)
        return [columns_of(keys, at, 1), columns_of(values, at, 1)]

    own = jnp.concatenate([piece for c in range(chunks) for piece in pair_of(c, 0)], axis=1)
    near = [[own] + [swap(jnp.concatenate(pair_of(c, r), axis=1), r) for r in range(1, group)] for c in range(chunks)]
    far_own = [upward(own, p) for p in range(before, 0, -1)]
    own_q = [[swap(columns_of(queries, c * group + (me ^ r), ratio), r) for r in range(group)] for c in range(chunks)]
    far = []
    for c in range(chunks):
        rest = jnp.concatenate(near[c][1:], axis=0)
        moved = [upward(rest, p) for p in range(before, 0, -1)]
        far.append([piece for pair in zip(far_own, moved) for piece in pair])

    padded = jnp.concatenate([jnp.full((before * group * rows,), -1, jnp.int32), episode])
    ids = lax.dynamic_slice_in_dim(padded, mine * group * rows, n_kv * rows, 0).reshape(n_kv, rows)
    first_id, last_id = ids[:, 0], ids[:, -1]
    at = before * group + (me ^ jnp.arange(group, dtype=jnp.int32))
    first = jnp.sum(last_id[None, :] < jnp.take(first_id, at)[:, None], axis=1, dtype=jnp.int32)
    first = jnp.clip(first, at - back, at)
    full = jnp.sum(first_id[None, :] < jnp.take(last_id, at)[:, None], axis=1, dtype=jnp.int32)
    full = jnp.maximum(full, at + 1 - WINDOW // rows)
    full = jnp.clip(full, first, at)
    meta = jnp.concatenate([me[None].astype(jnp.int32), first, full])
    qid = jnp.broadcast_to(ids[before * group :, :, None], (group, rows, HEAD_DIM))
    kid = ids[:, None, :]

    columns = out_weight.shape[1] // head_size
    targets = [(head + d) % head_size for d in list(range(1, head_size)) + [0]]
    sums, ready = [], []
    for c in range(chunks):
        mixed = [None] * group
        stride = 2 if SPLIT and group > 1 and c + 1 == chunks else 1
        for start in range(stride - 1, -1, -1):
            done = attend(
                meta, qid, kid, far[c], near[c], own_q[c][start::stride], c, group, before, back, start, stride
            )
            for r, piece in zip(range(start, group, stride), done):
                mixed[r] = swap(piece, r)
        if c + 1 < chunks:
            ahead = c + 1 if c + 2 == chunks else None
            made = project(me, targets, mixed, out_weight, c, columns, sums, jnp.float32, ahead)
            sums, ready = made[:head_size], made[head_size + 1 :]
    *sent, mixed = project(
        me, targets[:-1], mixed, out_weight, c, columns, sums[:-1], jnp.bfloat16, None, ready[:-1]
    )
    (kept,) = project(
        me, targets[-1:], [mixed], out_weight, c, columns, sums[-1:], jnp.bfloat16, None, ready[-1:]
    )
    for d in range(1, head_size):
        ring = [(s, (s + d) % head_size) for s in range(head_size)]
        sent[d - 1] = lax.ppermute(sent[d - 1], "head", ring)
    return add_up([kept, *sent])


def solution(mesh):
    placed = (P("seq", "head"), P("seq", "head"), P("seq", "head"), P(), P("head", None))
    return jax.shard_map(body, mesh=mesh, in_specs=placed, out_specs=P("seq", "head"), check_vma=False)
```

```python
import math

import jax
import jax.numpy as jnp
from jax import lax
from jax.experimental import pallas as pl
from jax.experimental.pallas import tpu as pltpu
from jax.sharding import PartitionSpec as P


HEAD_DIM = 128
WINDOW = 4096

SCORE_SCALE = math.log2(math.e) / 12.0
HIDDEN = -1e30
ATTEND_ROOM = 16 << 20
PROJECT_ROOM = 26 << 20
SPLIT = False


def plan(rows, kv_heads, seq_size, tokens):
    reach = min(WINDOW, tokens // 4)
    group = math.gcd(kv_heads, seq_size)
    group &= -group
    while group > 1 and group * rows > reach:
        group //= 2
    before = -(-(reach - 1) // (group * rows))
    back = -(-(reach - 1) // rows)
    return group, before, back


def attend_kernel(chunk, group, before, ratio, rows, start, stride, count, meta, qid, kid, *refs):
    n_kv = group * (before + 1)
    far, refs = refs[: 2 * before], refs[2 * before :]
    near, refs = refs[:group], refs[group:]
    q_in, refs = refs[:count], refs[count:]
    outs, refs = refs[:count], refs[count:]
    k_all, v_all, q_all, scores, top, acc = refs
    me = meta[0]
    base = before * group
    cut = rows // 2 if rows % (2 * HEAD_DIM) == 0 else rows

    def place(ref, row, column, slot):
        at = slice(row, row + rows)
        k_all[slot] = ref[at, column : column + HEAD_DIM]
        v_all[slot, :, :HEAD_DIM] = ref[at, column + HEAD_DIM : column + 2 * HEAD_DIM]

    own_column = chunk * 2 * HEAD_DIM
    earliest = meta[1 + start]
    for n in range(1, count):
        earliest = jnp.minimum(earliest, meta[1 + start + stride * n])
    for p in range(before):
        for r in range(group):
            slot = p * group + (me ^ r)

            @pl.when(slot >= earliest)
            def _():
                if r == 0:
                    place(far[2 * p], 0, own_column, slot)
                else:
                    place(far[2 * p + 1], (r - 1) * rows, 0, slot)

    for r in range(group):
        place(near[r], 0, 0 if r else own_column, base + (me ^ r))
    for n in range(count):
        q_all[n] = q_in[n][...]
    v_all[:, :, HEAD_DIM:] = jnp.ones((n_kv, rows, HEAD_DIM), jnp.bfloat16)

    def folded(s):
        parts = [s[:, n : n + HEAD_DIM] for n in range(0, s.shape[1], HEAD_DIM)]
        while len(parts) > 1:
            parts = [jnp.maximum(*parts[n : n + 2]) if n + 1 < len(parts) else parts[n] for n in range(0, len(parts), 2)]
        return parts[0]

    def one_block(n, carry):
        r = start + stride * n
        at = base + (me ^ r)
        first = meta[1 + r]
        full = meta[1 + group + r]

        def product(h, low, high, keys):
            q = q_all[n, low:high, h * HEAD_DIM : (h + 1) * HEAD_DIM]
            return lax.dot_general(q, keys, (((1,), (1,)), ((), ())), preferred_element_type=jnp.float32)

        def positions(low, high, wide):
            shape = (high - low, wide)
            q_pos = lax.broadcasted_iota(jnp.int32, shape, 0) + low
            return q_pos, lax.broadcasted_iota(jnp.int32, shape, 1)

        def same_episode(j, low, high, wide):
            own = jnp.concatenate([qid[me ^ r, low:high]] * (wide // HEAD_DIM), axis=1)
            return own == kid[j, :, :wide]

        for low in range(0, rows, cut):
            high = low + cut
            q_pos, k_pos = positions(low, high, high)
            seen = same_episode(at, low, high, high) & (k_pos <= q_pos)
            if rows > WINDOW:
                seen = seen & (k_pos - q_pos > -WINDOW)
            for h in range(ratio):
                s = jnp.where(seen, product(h, low, high, k_all[at, :high]), HIDDEN)
                scores[0, h, low:high, :high] = s
                top[h, low:high] = folded(s)

        def score(j, masked):
            keys = k_all[j]
            if masked:
                seen = same_episode(j, 0, rows, rows)
                if n_kv * rows > WINDOW:
                    q_pos, k_pos = positions(0, rows, rows)
                    seen = seen & (k_pos - q_pos > (at - j) * rows - WINDOW)
            for h in range(ratio):
                s = product(h, 0, rows, keys)
                if masked:
                    s = jnp.where(seen, s, HIDDEN)
                scores[at - j, h] = s
                top[h] = jnp.maximum(top[h], folded(s))

        def masked_step(j, c):
            score(j, True)
            return c

        def full_step(j, c):
            score(j, False)
            return c

        lax.fori_loop(first, full, masked_step, 0)
        lax.fori_loop(full, at, full_step, 0)
        for h in range(ratio):
            m = jnp.max(top[h], axis=1, keepdims=True) * SCORE_SCALE
            top[h] = jnp.broadcast_to(m, (rows, HEAD_DIM))

        def weighted(j, h, low, high, wide):
            m = jnp.concatenate([top[h, low:high]] * (wide // HEAD_DIM), axis=1)
            p = jnp.exp2(scores[at - j, h, low:high, :wide] * SCORE_SCALE - m).astype(jnp.bfloat16)
            return jnp.dot(p, v_all[j, :wide], preferred_element_type=jnp.float32)

        for h in range(ratio):
            for low in range(0, rows, cut):
                acc[h, low : low + cut] = weighted(at, h, low, low + cut, low + cut)

        def mix_step(j, c):
            for h in range(ratio):
                acc[h] += weighted(j, h, 0, rows, rows)
            return c

        def mix_two(n, c):
            j = first + 2 * n
            for h in range(ratio):
                acc[h] += weighted(j, h, 0, rows, rows) + weighted(j + 1, h, 0, rows, rows)
            return c

        pairs = lax.shift_right_logical(at - first, 1)
        lax.fori_loop(0, pairs, mix_two, 0)
        lax.fori_loop(first + 2 * pairs, at, mix_step, 0)
        for h in range(ratio):
            o = (acc[h, :, :HEAD_DIM] / acc[h, :, HEAD_DIM:]).astype(jnp.bfloat16)
            for k in range(count):

                @pl.when(n == k)
                def _():
                    outs[k][:, h * HEAD_DIM : (h + 1) * HEAD_DIM] = o

        return carry

    lax.fori_loop(0, count, one_block, 0)


def attend(meta, qid, kid, far, near, q, chunk, group, before, back, start, stride):
    rows, width = q[0].shape
    ratio = width // HEAD_DIM
    n_kv = (before + 1) * group
    count = len(q)
    vmem = pl.BlockSpec(memory_space=pltpu.VMEM)
    tiles = (back + 1) * ratio * rows * rows * 4
    return pl.pallas_call(
        lambda *refs: attend_kernel(chunk, group, before, ratio, rows, start, stride, count, *refs),
        out_shape=[jax.ShapeDtypeStruct((rows, width), jnp.bfloat16)] * count,
        in_specs=[pl.BlockSpec(memory_space=pltpu.SMEM)] + [vmem] * (2 + len(far) + len(near) + count),
        out_specs=[vmem] * count,
        scratch_shapes=[
            pltpu.VMEM((n_kv, rows, HEAD_DIM), jnp.bfloat16),
            pltpu.VMEM((n_kv, rows, 2 * HEAD_DIM), jnp.bfloat16),
            pltpu.VMEM((count, rows, width), jnp.bfloat16),
            pltpu.VMEM((back + 1, ratio, rows, rows), jnp.float32),
            pltpu.VMEM((ratio, rows, HEAD_DIM), jnp.float32),
            pltpu.VMEM((ratio, rows, 2 * HEAD_DIM), jnp.float32),
        ],
        compiler_params=pltpu.CompilerParams(vmem_limit_bytes=tiles + ATTEND_ROOM),
    )(meta, qid, kid, *far, *near, *q)


def project(me, targets, left, weight, chunk, columns, addends, dtype, ahead=None, ready=()):
    assembled = len(left) == 1
    group, rows, width = left[0].shape if assembled else (len(left), *left[0].shape)
    depth = group * width
    tile = max(t for t in range(128, 769, 128) if columns % t == 0)
    per = columns // tile
    count = len(targets)
    steps = count * per
    more = count if ahead is not None else 0

    def kernel(info, *refs):
        pieces, refs = refs[: len(left)], refs[len(left) :]
        w, refs = refs[: max(1, len(ready))], refs[max(1, len(ready)) :]
        added, refs = refs[: len(addends)], refs[len(addends) :]
        outs, (w_all, sem, sem_ahead) = refs[:-3], refs[-3:]
        lhs = pieces[0] if assembled else outs[count]

        def fetch(t, n):
            at = pl.ds(pl.multiple_of(info[1 + t] * columns + n * tile, 128), tile)
            slot = t * per + n
            source = w[0].at[pl.ds(chunk * depth, depth), at]
            return pltpu.make_async_copy(source, w_all.at[slot], sem.at[slot])

        def fetch_ahead(t):
            at = pl.ds(pl.multiple_of(info[1 + t] * columns, 128), columns)
            source = w[0].at[pl.ds(ahead * depth, depth), at]
            return pltpu.make_async_copy(source, outs[len(outs) - more + t], sem_ahead.at[t])

        if not ready:
            for t in range(count):
                for n in range(per):
                    fetch(t, n).start()
        for t in range(more):
            fetch_ahead(t).start()
        if not assembled:
            for r in range(group):
                lhs[info[0] ^ r] = pieces[r][...]
        for t in range(count):

            def step(n, carry):
                here = pl.ds(pl.multiple_of(n * tile, 128), tile)
                if ready:
                    w_tile = w[t][:, here]
                else:
                    fetch(t, n).wait()
                    w_tile = w_all[t * per + n]
                wide = jnp.concatenate([lhs[u] for u in range(group)], axis=1)
                total = jnp.dot(wide, w_tile, preferred_element_type=jnp.float32)
                if addends:
                    total = total + added[t][:, here]
                outs[t][:, here] = total.astype(dtype)
                return carry

            lax.fori_loop(0, per, step, 0)
        for t in range(more):
            fetch_ahead(t).wait()

    vmem = pl.BlockSpec(memory_space=pltpu.VMEM)
    hbm = pl.BlockSpec(memory_space=pltpu.HBM)
    shapes = [jax.ShapeDtypeStruct((rows, columns), dtype)] * count
    if not assembled:
        shapes.append(jax.ShapeDtypeStruct((group, rows, width), jnp.bfloat16))
    shapes += [jax.ShapeDtypeStruct((depth, columns), jnp.bfloat16)] * more
    return pl.pallas_call(
        kernel,
        out_shape=shapes,
        in_specs=[pl.BlockSpec(memory_space=pltpu.SMEM)]
        + [vmem] * len(left)
        + ([vmem] * len(ready) or [hbm])
        + [vmem] * len(addends),
        out_specs=[vmem] * len(shapes),
        scratch_shapes=[
            pltpu.VMEM((1, 16, 128) if ready else (steps, depth, tile), jnp.bfloat16),
            pltpu.SemaphoreType.DMA((steps,)),
            pltpu.SemaphoreType.DMA((max(1, more),)),
        ],
        compiler_params=pltpu.CompilerParams(vmem_limit_bytes=PROJECT_ROOM),
    )(jnp.stack([me, *targets]).astype(jnp.int32), *left, *(ready or [weight]), *addends)


def add_up(parts):
    rows, columns = parts[0].shape
    tile = max(t for t in range(8, 129, 8) if rows % t == 0)

    def kernel(*refs):
        out, held, sem = refs[-3:]

        def moved(n):
            at = pl.ds(pl.multiple_of(n * tile, 8), tile)
            return pltpu.make_async_copy(held.at[at], out.at[at], sem.at[n])

        def step(n, carry):
            at = pl.ds(pl.multiple_of(n * tile, 8), tile)
            total = refs[0][at].astype(jnp.float32)
            for ref in refs[1:-3]:
                total = total + ref[at].astype(jnp.float32)
            held[at] = total.astype(jnp.bfloat16)
            moved(n).start()
            return carry

        lax.fori_loop(0, rows // tile, step, 0)
        for n in range(rows // tile):
            moved(n).wait()

    return pl.pallas_call(
        kernel,
        out_shape=jax.ShapeDtypeStruct((rows, columns), jnp.bfloat16),
        in_specs=[pl.BlockSpec(memory_space=pltpu.VMEM)] * len(parts),
        out_specs=pl.BlockSpec(memory_space=pltpu.HBM),
        scratch_shapes=[
            pltpu.VMEM((rows, columns), jnp.bfloat16),
            pltpu.SemaphoreType.DMA((rows // tile,)),
        ],
        compiler_params=pltpu.CompilerParams(vmem_limit_bytes=12 << 20),
    )(*parts)


def body(queries, keys, values, episode, out_weight):
    rows = queries.shape[0]
    tokens = episode.shape[0]
    seq_size = lax.axis_size("seq")
    head_size = lax.axis_size("head")
    kv_heads = keys.shape[1] // HEAD_DIM
    ratio = queries.shape[1] // keys.shape[1]
    group, before, back = plan(rows, kv_heads, seq_size, tokens)
    chunks = kv_heads // group
    me = lax.axis_index("seq") % group
    mine = lax.axis_index("seq") // group
    head = lax.axis_index("head")
    n_kv = (before + 1) * group

    def swap(value, r):
        if not r:
            return value
        return lax.ppermute(value, "seq", [(s, s ^ r) for s in range(seq_size)])

    def upward(value, p):
        step = p * group
        return lax.ppermute(value, "seq", [(s, s + step) for s in range(seq_size - step)])

    def columns_of(value, at, heads):
        return lax.dynamic_slice_in_dim(value, at * heads * HEAD_DIM, heads * HEAD_DIM, 1)

    def pair_of(c, r):
        at = c * group + (me ^ r)
        return [columns_of(keys, at, 1), columns_of(values, at, 1)]

    own = jnp.concatenate([piece for c in range(chunks) for piece in pair_of(c, 0)], axis=1)
    pieces = [[jnp.concatenate(pair_of(c, r), axis=1) for r in range(1, group)] for c in range(chunks)]
    near = [[own] + [swap(piece, r + 1) for r, piece in enumerate(pieces[c])] for c in range(chunks)]
    far_own = [upward(own, p) for p in range(before, 0, -1)]
    own_q = [[swap(columns_of(queries, c * group + (me ^ r), ratio), r) for r in range(group)] for c in range(chunks)]
    far = []
    for c in range(chunks):
        rest = jnp.concatenate(near[c][1:], axis=0) if group > 1 else own
        moved = [upward(rest, p) for p in range(before, 0, -1)]
        far.append([piece for pair in zip(far_own, moved) for piece in pair])

    padded = jnp.concatenate([jnp.full((before * group * rows,), -1, jnp.int32), episode])
    ids = lax.dynamic_slice_in_dim(padded, mine * group * rows, n_kv * rows, 0).reshape(n_kv, rows)
    first_id, last_id = ids[:, 0], ids[:, -1]
    at = before * group + (me ^ jnp.arange(group, dtype=jnp.int32))
    first = jnp.sum(last_id[None, :] < jnp.take(first_id, at)[:, None], axis=1, dtype=jnp.int32)
    first = jnp.clip(first, at - back, at)
    full = jnp.sum(first_id[None, :] < jnp.take(last_id, at)[:, None], axis=1, dtype=jnp.int32)
    full = jnp.maximum(full, at + 1 - WINDOW // rows)
    full = jnp.clip(full, first, at)
    meta = jnp.concatenate([me[None].astype(jnp.int32), first, full])
    qid = jnp.broadcast_to(ids[before * group :, :, None], (group, rows, HEAD_DIM))
    kid = ids[:, None, :]

    columns = out_weight.shape[1] // head_size
    targets = [(head + d) % head_size for d in list(range(1, head_size)) + [0]]
    sums, ready = [], []
    for c in range(chunks):
        mixed = [None] * group
        stride = 2 if SPLIT and group > 1 and c + 1 == chunks else 1
        for start in range(stride - 1, -1, -1):
            done = attend(
                meta, qid, kid, far[c], near[c], own_q[c][start::stride], c, group, before, back, start, stride
            )
            for r, piece in zip(range(start, group, stride), done):
                mixed[r] = swap(piece, r)
        if c + 1 < chunks:
            ahead = c + 1 if c + 2 == chunks else None
            made = project(me, targets, mixed, out_weight, c, columns, sums, jnp.float32, ahead)
            sums, ready = made[:head_size], made[head_size + 1 :]
    *sent, mixed = project(
        me, targets[:-1], mixed, out_weight, c, columns, sums[:-1], jnp.bfloat16, None, ready[:-1]
    )
    (kept,) = project(
        me, targets[-1:], [mixed], out_weight, c, columns, sums[-1:], jnp.bfloat16, None, ready[-1:]
    )
    for d in range(1, head_size):
        ring = [(s, (s + d) % head_size) for s in range(head_size)]
        sent[d - 1] = lax.ppermute(sent[d - 1], "head", ring)
    return add_up([kept, *sent])


def solution(mesh):
    placed = (P("seq", "head"), P("seq", "head"), P("seq", "head"), P(), P("head", None))
    return jax.shard_map(body, mesh=mesh, in_specs=placed, out_specs=P("seq", "head"), check_vma=False)
```
